32 devices in a mesh: term: 8 (over z, core), sector: 4 (over y, x).
Axes of the slice: x: 2, y: 2, z: 4, core: 2. Of those that a mesh axis runs over, the one named last changes fastest.
Arguments:
- wavefunction: bfloat16 [24, 256, 256], P('sector'), may hold values from -6 to 6
- left_env: bfloat16 [24, 24, 256, 256], P('term', 'sector')
- right_env: bfloat16 [24, 24, 256, 256], P('term', 'sector')
- source: int32 [24, 24], P('term'), may hold values from 0 to 23, as said below
- block_size: int32 [24, 2], P('sector'), may hold values from 32 to 256
Outputs:
- first_product: float32 [24, 256, 256], P('sector', 'term')
- second_product: float32 [24, 256, 256], P('sector', 'term')
The draws below stay inside these ranges and needn't reach their ends.
Inputs may be any that keep to these rules, and one draw needn't show every extreme that they name: Owner of sector s is s // 6. Among the 3 x 6 entries of source in one device's rows (one index of term) and columns (one index of sector), at most 5 name sectors of any one owner, and some owner is named exactly 5 times.
All inputs are finite; a program needn't handle non-finite values.
Results may differ from the reference program's by a relative error of at most 0.0037.
Values may be sent and summed in bfloat16 or wider, within the bound.
A program may use at most 64 MiB of HBM per device.

```python
import math
import jax
import jax.numpy as jnp
from jax import lax

DL = 256
SEC_DEV = 6
B_DEV = 3
SECTORS = 24
BONDS = 24
CAP = 5


def environment(key, salt):
    base = jax.random.fold_in(key, salt)
    diagonal = jax.random.uniform(jax.random.fold_in(base, 1), (BONDS, SECTORS, DL), jnp.float32, 0.2, 1.2)
    noise = jax.random.normal(jax.random.fold_in(base, 2), (BONDS, SECTORS, DL, DL), jnp.float32)
    identity_table = jnp.eye(DL, dtype=jnp.float32)
    matrix = (noise * (0.6 / math.sqrt(DL)) + diagonal[..., None] * identity_table) / math.sqrt(BONDS)
    return matrix.astype(jnp.bfloat16)


def draw_left_env(key, part):
    return environment(key, 101)


def draw_right_env(key, part):
    return environment(key, 202)


def draw_source(key, part):
    term_groups = BONDS // B_DEV
    sector_groups = SECTORS // SEC_DEV
    item_count = B_DEV * SEC_DEV
    base = jax.random.fold_in(key, 303)

    def one_block(number):
        block_key = jax.random.fold_in(base, number)
        order = jax.random.permutation(jax.random.fold_in(block_key, 1), item_count)
        owners = jax.random.permutation(jax.random.fold_in(block_key, 2), sector_groups)
        owner_of = owners[order // CAP]
        local_slot = jax.random.randint(jax.random.fold_in(block_key, 3), (item_count,), 0, SEC_DEV)
        return (owner_of * SEC_DEV + local_slot).astype(jnp.int32)
    blocks = jax.vmap(one_block)(jnp.arange(term_groups * sector_groups, dtype=jnp.int32))
    blocks = blocks.reshape(term_groups, sector_groups, B_DEV, SEC_DEV).transpose(0, 2, 1, 3)
    return blocks.reshape(BONDS, SECTORS)


def plant(array, own_key, smallest, high):
    dims = array.shape
    spot = [jax.random.randint(jax.random.fold_in(own_key, axis), (), 0, dims[axis]) for axis in range(len(dims))]
    array = array.at[tuple(spot)].set(smallest)
    longest = dims.index(max(dims))
    spot[longest] = (spot[longest] + 1) % dims[longest]
    return array.at[tuple(spot)].set(high)


def block_scale(stream_key, shape, split, low, largest):
    level, own = 1.0, jax.random.fold_in(stream_key, 6)
    for axis_at, shards_of in split:
        steps = jnp.exp(jax.random.uniform(jax.random.fold_in(own, axis_at), (shards_of,), jnp.float32, low / len(split), largest / len(split)))
        level = level * jnp.repeat(steps, shape[axis_at] // shards_of).reshape([-1 if axis == axis_at else 1 for axis in range(len(shape))])
    return level


def centred(stream_key, dims, scale, bound, shards=(), kind=jnp.bfloat16):
    drawn = scale * jax.random.normal(stream_key, dims, jnp.float32)
    if shards:
        drawn = drawn * block_scale(stream_key, dims, shards, -0.22, 0.18)
    return jnp.clip(drawn, -bound, bound).astype(kind)


def setup_inputs(seed: int = 0) -> dict:
    arg_keys = jax.random.split(jax.random.key(seed), 6)
    return {
        "wavefunction": centred(arg_keys[0], (SECTORS, DL, DL), 1.0, 6.0, ((0, 4),)),
        "left_env": draw_left_env(jax.random.fold_in(arg_keys[5], 71), 0),
        "right_env": draw_right_env(jax.random.fold_in(arg_keys[5], 71), 0),
        "source": draw_source(jax.random.fold_in(arg_keys[5], 71), 0),
        "block_size": plant(jax.random.randint(arg_keys[4], (SECTORS, 2), DL // 8, DL + 1), jax.random.fold_in(arg_keys[4], 1), DL // 8, DL).astype(jnp.int32),
    }


epsilon = 1e-06

def block_mask(block_size, width):
    positions = jnp.arange(width, dtype=jnp.int32)
    row_keep = positions[None, :] < block_size[:, 0:1]
    column_keep = positions[None, :] < block_size[:, 1:2]
    return row_keep[:, :, None] & column_keep[:, None, :]

def apply_operator(vector, left_env, right_env, source, keep):
    masked = jnp.where(keep, vector, jnp.zeros_like(vector))

    def one_bond(summed, inputs):
        left_bond, right_bond, source_bond = inputs
        picked = jnp.take(masked, source_bond.astype(jnp.int32), axis=0)
        half_product = jnp.einsum('kij,kjl->kil', left_bond.astype(jnp.float32), picked.astype(jnp.float32)).astype(jnp.bfloat16)
        bond_term = jnp.einsum('kil,kml->kim', half_product.astype(jnp.float32), right_bond.astype(jnp.float32))
        return (summed + bond_term, None)
    initial = jnp.zeros(masked.shape, jnp.float32)
    summed, _ = lax.scan(one_bond, initial, (left_env, right_env, source))
    return (jnp.where(keep, summed, jnp.zeros_like(summed)), masked)

def reference(wavefunction, left_env, right_env, source, block_size):
    keep = block_mask(block_size, DL)
    first_product, masked = apply_operator(wavefunction, left_env, right_env, source, keep)
    masked_float = masked.astype(jnp.float32)
    margin = jnp.sum(masked_float * first_product)
    self_norm = jnp.sum(masked_float * masked_float)
    residual = first_product - margin / self_norm * masked_float
    spread = jnp.sum(residual * residual)
    next_vector = (residual * lax.rsqrt(spread / (SECTORS * DL * DL) + epsilon)).astype(jnp.bfloat16)
    second_product, _ = apply_operator(next_vector, left_env, right_env, source, keep)
    return (first_product, second_product)
```

```python
import functools

import jax
import jax.numpy as jnp
from jax import lax
from jax.experimental import pallas as pl
from jax.experimental.pallas import tpu as pltpu
from jax.sharding import PartitionSpec as P

epsilon = 1e-06
MESH = pl.DeviceIdType.MESH
LANES = 128


def grid_of(sector_count):
    across = 1
    while across * across * 2 <= sector_count:
        across *= 2
    while sector_count % across:
        across -= 1
    return across, sector_count // across


def fold(values):
    rows = values.reshape(-1, 8, values.shape[-1])
    total = jnp.sum(rows, axis=0)
    parts = [total[:, i : i + LANES] for i in range(0, total.shape[1], LANES)]
    return functools.reduce(lambda a, b: a + b, parts)


def kernel(
    dims,
    source_ref,
    size_ref,
    wave_hbm,
    left_hbm,
    right_hbm,
    first_ref,
    second_ref,
    wave,
    left,
    right,
    pool,
    partial,
    from_core,
    chip_sum,
    from_line,
    term_out,
    term_in,
    sector_out,
    sector_in,
    load_sem,
    send_sem,
    net_sem,
    core_sem,
    pair_send,
    pair_recv,
    line_send,
    line_recv,
    term_send,
    term_recv,
    sector_send,
    sector_recv,
):
    terms, sectors, blocks, bonds, width = dims
    line = terms // 2
    rows = width // terms
    group = 2 if blocks % 2 == 0 else 1
    groups = blocks // group
    nx, ny = grid_of(sectors)
    t = lax.axis_index("term")
    s = lax.axis_index("sector")
    c = lax.rem(t, 2)
    z = lax.div(t, 2)
    x = lax.rem(s, nx)
    y = lax.div(s, nx)
    other = t + 1 - 2 * c

    def sector_at(a, b):
        if nx == ny:
            dx = a * (1 - c) + b * c
            dy = b * (1 - c) + a * c
        else:
            dx, dy = a, b
        return lax.rem(y + dy, ny) * nx + lax.rem(x + dx, nx)

    def z_at(j):
        return lax.rem(z + j, line)

    loads = [
        pltpu.make_async_copy(wave_hbm, wave, load_sem.at[0]),
        pltpu.make_async_copy(left_hbm, left, load_sem.at[1]),
        pltpu.make_async_copy(right_hbm, right, load_sem.at[2]),
    ]
    for copy in loads:
        copy.start()

    barrier = pltpu.get_barrier_semaphore()
    for j in range(1, terms):
        pl.semaphore_signal(
            barrier, inc=1, device_id=(lax.rem(t + j, terms), s), device_id_type=MESH
        )
    for j in range(1, sectors):
        pl.semaphore_signal(
            barrier, inc=1, device_id=(t, lax.rem(s + j, sectors)), device_id_type=MESH
        )

    row_at = lax.broadcasted_iota(jnp.int32, (width, width), 0)
    column_at = lax.broadcasted_iota(jnp.int32, (width, width), 1)

    def keep_of(k):
        return (row_at < size_ref[k, 0]) & (column_at < size_ref[k, 1])

    loads[0].wait()
    for k in range(blocks):
        pool[0, s * blocks + k] = jnp.where(keep_of(k), wave[k], jnp.zeros_like(wave[k]))

    pl.semaphore_wait(barrier, terms + sectors - 2)

    sent = []

    def send(stage, region, slot, target, by_core):
        number = len(sent)
        copy = pltpu.make_async_remote_copy(
            src_ref=region,
            dst_ref=region,
            send_sem=send_sem.at[number],
            recv_sem=(core_sem if by_core else net_sem).at[stage, slot],
            device_id=target,
            device_id_type=MESH,
        )
        copy.start()
        sent.append(copy)

    def arrived(stage, region, slot, by_core):
        pltpu.make_async_remote_copy(
            src_ref=region,
            dst_ref=region,
            send_sem=send_sem.at[0],
            recv_sem=(core_sem if by_core else net_sem).at[stage, slot],
            device_id=(other, s),
            device_id_type=MESH,
        ).wait_recv()

    def gather(stage, region_of, z_order):
        def spread_out(piece, zz, to_first, to_second, to_core):
            region = region_of(piece, zz, c)
            slot = zz * sectors + piece
            if to_second:
                for b in range(1, ny):
                    send(stage, region, slot, (t, sector_at(0, b)), False)
            if to_first:
                for a in range(1, nx):
                    send(stage, region, slot, (t, sector_at(a, 0)), False)
            if to_core:
                send(stage, region, slot, (other, s), True)

        def land(piece, zz):
            arrived(stage, region_of(piece, zz, c), zz * sectors + piece, False)

        def firsts(j):
            for a in range(1, nx):
                piece = sector_at(a, 0)
                land(piece, z_at(j))
                spread_out(piece, z_at(j), False, True, True)

        def seconds(j):
            for a in range(nx):
                for b in range(1, ny):
                    piece = sector_at(a, b)
                    land(piece, z_at(j))
                    spread_out(piece, z_at(j), False, False, True)

        for i, j in enumerate(z_order):
            if i == 0:
                for jj in z_order[1:]:
                    region = region_of(s, z, c)
                    send(stage, region, z * sectors + s, (2 * z_at(jj) + c, s), False)
                spread_out(s, z, True, True, len(z_order) > 1)
            else:
                land(s, z_at(j))
                spread_out(s, z_at(j), True, True, True)
                firsts(z_order[i - 1])
        firsts(z_order[-1])
        for j in z_order:
            seconds(j)
        for j in z_order:
            for a in range(nx):
                for b in range(ny):
                    if a or b or len(z_order) > 1:
                        piece = sector_at(a, b)
                        arrived(
                            stage,
                            region_of(piece, z_at(j), 1 - c),
                            z_at(j) * sectors + piece,
                            True,
                        )
        for copy in sent:
            copy.wait_send()
        sent.clear()

    def wave_region(piece, zz, core):
        half = width // 2
        return pool.at[
            0, pl.ds(piece * blocks, blocks), pl.ds(pl.multiple_of(core * half, half), half), :
        ]

    def next_region(piece, zz, core):
        return pool.at[
            1,
            pl.ds(piece * blocks, blocks),
            pl.ds(pl.multiple_of((2 * zz + core) * rows, rows), rows),
            :,
        ]

    def pair_copy(stage, g):
        span = pl.ds(g * group, group)
        return pltpu.make_async_remote_copy(
            src_ref=partial.at[stage, span, :, 1 - c],
            dst_ref=from_core.at[stage, span],
            send_sem=pair_send.at[stage, g],
            recv_sem=pair_recv.at[stage, g],
            device_id=(other, s),
            device_id_type=MESH,
        )

    def line_copy(stage, g, j):
        span = pl.ds(g * group, group)
        return pltpu.make_async_remote_copy(
            src_ref=chip_sum.at[stage, z_at(j), span],
            dst_ref=from_line.at[stage, z, span],
            send_sem=line_send.at[stage, g, j],
            recv_sem=line_recv.at[stage, g, z],
            device_id=(2 * z_at(j) + c, s),
            device_id_type=MESH,
        )

    def line_landed(stage, g, j):
        span = pl.ds(g * group, group)
        pltpu.make_async_remote_copy(
            src_ref=chip_sum.at[stage, z, span],
            dst_ref=from_line.at[stage, z_at(j), span],
            send_sem=line_send.at[stage, g, j],
            recv_sem=line_recv.at[stage, g, z_at(j)],
            device_id=(2 * z_at(j) + c, s),
            device_id_type=MESH,
        ).wait_recv()

    def operate(stage, with_sums):
        def finish(g):
            pair_copy(stage, g).wait_recv()
            for i in range(group):
                k = g * group + i
                both = partial[stage, k, :, pl.ds(c, 1)].reshape(line, rows, width)
                both = both + from_core[stage, k]
                chip_sum[stage, :, k] = both.astype(jnp.bfloat16)
            for j in range(1, line):
                line_copy(stage, g, j).start()

        def step(g, sums):
            for i in range(group):
                k = g * group + i
                total = None
                for b in range(bonds):
                    picked = pool[stage, source_ref[b, s * blocks + k]]
                    half = jnp.dot(
                        left[b, k], picked, preferred_element_type=jnp.float32
                    ).astype(jnp.bfloat16)
                    term = lax.dot_general(
                        half,
                        right[b, k],
                        (((1,), (1,)), ((), ())),
                        preferred_element_type=jnp.float32,
                    )
                    total = term if total is None else total + term
                total = jnp.where(keep_of(k), total, jnp.zeros_like(total))
                if with_sums:
                    own = pool[0, s * blocks + k].astype(jnp.float32)
                    sums = (sums[0] + fold(total * own), sums[1] + fold(total * total))
                partial[stage, k] = total.reshape(line, 2, rows, width)
            pair_copy(stage, g).start()

            @pl.when(g > 0)
            def _():
                finish(g - 1)

            return sums

        zero = jnp.zeros((8, LANES), jnp.float32)
        sums = lax.fori_loop(0, groups, step, (zero, zero) if with_sums else (zero,))
        return sums, functools.partial(finish, groups - 1)

    def collect(stage):
        for g in range(groups):
            for j in range(1, line):
                line_landed(stage, g, j)
        mine = partial[stage, :, pl.ds(z, 1), pl.ds(c, 1)].reshape(blocks, rows, width)
        mine = mine + from_core[stage, :, pl.ds(z, 1)].reshape(blocks, rows, width)
        for j in range(1, line):
            piece = from_line[stage, pl.ds(z_at(j), 1)].reshape(blocks, rows, width)
            mine = mine + piece.astype(jnp.float32)
        for g in range(groups):
            pair_copy(stage, g).wait_send()
            for j in range(1, line):
                line_copy(stage, g, j).wait_send()
        return mine

    def term_copy(stage, j):
        return pltpu.make_async_remote_copy(
            src_ref=term_out.at[stage],
            dst_ref=term_in.at[stage, j],
            send_sem=term_send.at[stage, j],
            recv_sem=term_recv.at[stage, j],
            device_id=(lax.rem(t + j, terms), s),
            device_id_type=MESH,
        )

    def sector_copy(stage, j):
        return pltpu.make_async_remote_copy(
            src_ref=sector_out.at[stage],
            dst_ref=sector_in.at[stage, j],
            send_sem=sector_send.at[stage, j],
            recv_sem=sector_recv.at[stage, j],
            device_id=(t, lax.rem(s + j, sectors)),
            device_id_type=MESH,
        )

    def share_start(stage, tiles):
        for i, tile in enumerate(tiles):
            term_out[stage, i] = tile
        for j in range(1, terms):
            term_copy(stage, j).start()

    def share_turn(stage):
        value = term_out[stage]
        for j in range(1, terms):
            term_copy(stage, j).wait_recv()
            value = value + term_in[stage, j]
        sector_out[stage] = value
        for j in range(1, sectors):
            sector_copy(stage, j).start()

    def share_end(stage):
        value = sector_out[stage]
        for j in range(1, sectors):
            sector_copy(stage, j).wait_recv()
            value = value + sector_in[stage, j]
        for j in range(1, terms):
            term_copy(stage, j).wait_send()
        for j in range(1, sectors):
            sector_copy(stage, j).wait_send()
        return jnp.sum(jnp.sum(value, axis=2, keepdims=True), axis=1, keepdims=True)

    gather(0, wave_region, [0])
    loads[1].wait()
    loads[2].wait()

    sums, last = operate(0, True)
    my_rows = pl.ds(pl.multiple_of(t * rows, rows), rows)
    own = pool[0, pl.ds(s * blocks, blocks), my_rows, :].astype(jnp.float32)
    share_start(0, (sums[0], sums[1], fold(own * own)))
    last()
    share_turn(0)
    first = collect(0)
    first_ref[...] = first
    whole = share_end(0)
    count = float(sectors * blocks * width * width)
    ratio = whole[0:1] / whole[2:3]
    early = jnp.maximum(lax.rsqrt(whole[1:2] / count + epsilon), 1e-18)
    residual = first - ratio * own
    pool[1, pl.ds(s * blocks, blocks), my_rows, :] = (residual * early).astype(jnp.bfloat16)
    zero = jnp.zeros((8, LANES), jnp.float32)
    gather(1, next_region, [0] + [j for i in range(1, line) for j in sorted({i, line - i}) if i <= line - i])
    share_start(1, (fold(residual * residual), zero, zero))

    _, last = operate(1, False)
    last()
    share_turn(1)
    second = collect(1)
    spread = share_end(1)[0:1]
    second_ref[...] = second * (lax.rsqrt(spread / count + epsilon) / early)


def body(dims, wavefunction, left_env, right_env, source, block_size):
    terms, sectors, blocks, bonds, width = dims
    line = terms // 2
    rows = width // terms
    groups = blocks // (2 if blocks % 2 == 0 else 1)
    nx, ny = grid_of(sectors)
    piece = jax.ShapeDtypeStruct((blocks, rows, width), jnp.float32)
    dma = pltpu.SemaphoreType.DMA
    pieces = line * sectors
    sends = line * (nx - 1 + nx * (ny - 1) + sectors) + line
    return pl.pallas_call(
        functools.partial(kernel, dims),
        out_shape=(piece, piece),
        in_specs=[pl.BlockSpec(memory_space=pltpu.SMEM)] * 2
        + [pl.BlockSpec(memory_space=pl.ANY)] * 3,
        out_specs=(pl.BlockSpec(memory_space=pltpu.VMEM),) * 2,
        scratch_shapes=[
            pltpu.VMEM((blocks, width, width), jnp.bfloat16),
            pltpu.VMEM((bonds, blocks, width, width), jnp.bfloat16),
            pltpu.VMEM((bonds, blocks, width, width), jnp.bfloat16),
            pltpu.VMEM((2, sectors * blocks, width, width), jnp.bfloat16),
            pltpu.VMEM((2, blocks, line, 2, rows, width), jnp.float32),
            pltpu.VMEM((2, blocks, line, rows, width), jnp.float32),
            pltpu.VMEM((2, line, blocks, rows, width), jnp.bfloat16),
            pltpu.VMEM((2, line, blocks, rows, width), jnp.bfloat16),
            pltpu.VMEM((2, 3, 8, LANES), jnp.float32),
            pltpu.VMEM((2, terms, 3, 8, LANES), jnp.float32),
            pltpu.VMEM((2, 3, 8, LANES), jnp.float32),
            pltpu.VMEM((2, sectors, 3, 8, LANES), jnp.float32),
            dma((3,)),
            dma((sends,)),
            dma((2, pieces)),
            dma((2, pieces)),
            dma((2, groups)),
            dma((2, groups)),
            dma((2, groups, line)),
            dma((2, groups, line)),
            dma((2, terms)),
            dma((2, terms)),
            dma((2, sectors)),
            dma((2, sectors)),
        ],
        compiler_params=pltpu.CompilerParams(
            collective_id=0, has_side_effects=True, vmem_limit_bytes=60 * 1024 * 1024
        ),
    )(source, block_size, wavefunction, left_env, right_env)


def solution(mesh):
    terms, sectors = mesh.shape["term"], mesh.shape["sector"]

    def local(wavefunction, left_env, right_env, source, block_size):
        blocks, width = wavefunction.shape[0], wavefunction.shape[1]
        dims = (terms, sectors, blocks, source.shape[0], width)
        return body(dims, wavefunction, left_env, right_env, source, block_size)

    placed = (
        P("sector", None, None),
        P("term", "sector", None, None),
        P("term", "sector", None, None),
        P("term", None),
        P("sector", None),
    )
    return jax.shard_map(
        local,
        mesh=mesh,
        in_specs=placed,
        out_specs=(P("sector", "term", None), P("sector", "term", None)),
        check_vma=False,
    )
```

```python
import functools

import jax
import jax.numpy as jnp
from jax import lax
from jax.experimental import pallas as pl
from jax.experimental.pallas import tpu as pltpu
from jax.sharding import PartitionSpec as P

epsilon = 1e-06
MESH = pl.DeviceIdType.MESH
LANES = 128
SHARED = 1
CUTS = 2
GROUP = 1
LAG = 3


def grid_of(sector_count):
    across = 1
    while across * across * 2 <= sector_count:
        across *= 2
    while sector_count % across:
        across -= 1
    return across, sector_count // across


def fold(values):
    rows = values.reshape(-1, 8, values.shape[-1])
    total = jnp.sum(rows, axis=0)
    parts = [total[:, i : i + LANES] for i in range(0, total.shape[1], LANES)]
    return functools.reduce(lambda a, b: a + b, parts)


def kernel(
    dims,
    source_ref,
    size_ref,
    wave_hbm,
    left_hbm,
    right_hbm,
    first_ref,
    second_ref,
    wave,
    left,
    right,
    pool,
    partial,
    from_core,
    chip_sum,
    from_line,
    term_out,
    term_in,
    sector_out,
    sector_in,
    load_sem,
    send_sem,
    net_sem,
    core_sem,
    pair_send,
    pair_recv,
    line_send,
    line_recv,
    term_send,
    term_recv,
    sector_send,
    sector_recv,
):
    terms, sectors, blocks, bonds, width = dims
    line = terms // 2
    rows = width // terms
    group = GROUP if blocks % GROUP == 0 else 1
    groups = blocks // group
    nx, ny = grid_of(sectors)
    t = lax.axis_index("term")
    s = lax.axis_index("sector")
    c = lax.rem(t, 2)
    z = lax.div(t, 2)
    x = lax.rem(s, nx)
    y = lax.div(s, nx)
    other = t + 1 - 2 * c

    def sector_at(a, b):
        if nx == ny:
            dx = a * (1 - c) + b * c
            dy = b * (1 - c) + a * c
        else:
            dx, dy = a, b
        return lax.rem(y + dy, ny) * nx + lax.rem(x + dx, nx)

    def z_at(j):
        return lax.rem(z + j, line)

    loads = [
        pltpu.make_async_copy(wave_hbm, wave, load_sem.at[0]),
        pltpu.make_async_copy(left_hbm, left, load_sem.at[1]),
        pltpu.make_async_copy(right_hbm, right, load_sem.at[2]),
    ]
    for copy in loads:
        copy.start()

    barrier = pltpu.get_barrier_semaphore()
    for j in range(1, terms):
        pl.semaphore_signal(
            barrier, inc=1, device_id=(lax.rem(t + j, terms), s), device_id_type=MESH
        )
    for j in range(1, sectors):
        pl.semaphore_signal(
            barrier, inc=1, device_id=(t, lax.rem(s + j, sectors)), device_id_type=MESH
        )

    row_at = lax.broadcasted_iota(jnp.int32, (width, width), 0)
    column_at = lax.broadcasted_iota(jnp.int32, (width, width), 1)

    def keep_of(k):
        return (row_at < size_ref[0, k]) & (column_at < size_ref[1, k])

    loads[0].wait()
    for k in range(blocks):
        pool[0, s * blocks + k] = jnp.where(keep_of(k), wave[k], jnp.zeros_like(wave[k]))

    pl.semaphore_wait(barrier, terms + sectors - 2)

    sent = []

    def send(stage, region, slot, target, by_core, condition=None):
        number = len(sent)

        def make():
            return pltpu.make_async_remote_copy(
                src_ref=region,
                dst_ref=region,
                send_sem=send_sem.at[number],
                recv_sem=(core_sem if by_core else net_sem).at[stage, slot],
                device_id=target,
                device_id_type=MESH,
            )

        when(condition, lambda: make().start())
        sent.append((condition, make))

    def when(condition, action):
        if condition is None:
            action()
        else:
            pl.when(condition)(action)

    def arrived(stage, region, slot, by_core):
        pltpu.make_async_remote_copy(
            src_ref=region,
            dst_ref=region,
            send_sem=send_sem.at[0],
            recv_sem=(core_sem if by_core else net_sem).at[stage, slot],
            device_id=(other, s),
            device_id_type=MESH,
        ).wait_recv()

    def drain():
        for condition, make in sent:
            when(condition, lambda make=make: make().wait_send())
        sent.clear()

    elsewhere = [(a, b) for a in range(nx) for b in range(ny) if a or b]

    def gather_wave():
        half = width // 2
        shared = SHARED if line % 2 == 0 and blocks > 2 * SHARED else 0
        parity = lax.rem(z, 2)
        mate = z + 1 - 2 * parity
        common = [parity * shared + i for i in range(shared)]
        theirs = [(1 - parity) * shared + i for i in range(shared)]
        alone = list(range(2 * shared, blocks))

        def region_of(piece, k, core):
            return pool.at[
                0, piece * blocks + k, pl.ds(pl.multiple_of(core * half, half), half), :
            ]

        def put(piece, k, to_first=False, to_second=False, to_mate=False, to_core=False):
            region, slot = region_of(piece, k, c), piece * blocks + k
            if to_second:
                for b in range(1, ny):
                    send(0, region, slot, (t, sector_at(0, b)), False)
            if to_first:
                for a in range(1, nx):
                    send(0, region, slot, (t, sector_at(a, 0)), False)
            if to_mate:
                send(0, region, slot, (2 * mate + c, s), False)
            if to_core:
                send(0, region, slot, (other, s), True)

        def pass_on(spots, ks, **where):
            for k in ks:
                for a, b in spots:
                    piece = sector_at(a, b)
                    arrived(0, region_of(piece, k, c), piece * blocks + k, False)
                    put(piece, k, **where)

        side_one = [(a, 0) for a in range(1, nx)]
        side_two = [(0, b) for b in range(1, ny)]
        corners = [(a, b) for a in range(1, nx) for b in range(1, ny)]
        for k in common:
            put(s, k, to_first=True, to_second=True)
        for k in alone:
            put(s, k, to_first=True)
        pass_on(side_one, common, to_second=True, to_mate=True, to_core=True)
        for k in alone:
            put(s, k, to_second=True)
        pass_on(side_two, common, to_mate=True, to_core=True)
        pass_on(side_one, alone[:1], to_second=True, to_core=True)
        pass_on(corners, common, to_mate=True, to_core=True)
        pass_on(side_one, alone[1:], to_second=True, to_core=True)
        pass_on(side_two, alone, to_core=True)
        pass_on(side_one + side_two, theirs, to_core=True)
        pass_on(corners, theirs, to_core=True)
        pass_on(corners, alone, to_core=True)
        for k in range(blocks):
            for a, b in elsewhere:
                piece = sector_at(a, b)
                arrived(0, region_of(piece, k, 1 - c), piece * blocks + k, True)
        drain()

    def gather_next():
        cuts = CUTS if blocks % CUTS == 0 else 1
        deep = blocks // cuts

        def region_of(piece, zz, q, core):
            return pool.at[
                1,
                pl.ds(piece * blocks + q * deep, deep),
                pl.ds(pl.multiple_of((2 * zz + core) * rows, rows), rows),
                :,
            ]

        def slot_of(piece, zz, q):
            return (zz * sectors + piece) * cuts + q

        def put(piece, zz, q, valid, to_line=(), to_first=False, to_second=False):
            region, slot = region_of(piece, zz, q, c), slot_of(piece, zz, q)
            for step in to_line:
                inside = (z + step >= 0) & (z + step < line)
                inside = inside if valid is None else inside & valid
                send(1, region, slot, (2 * (z + step) + c, s), False, inside)
            if to_second:
                for b in range(1, ny):
                    send(1, region, slot, (t, sector_at(0, b)), False, valid)
            if to_first:
                for a in range(1, nx):
                    send(1, region, slot, (t, sector_at(a, 0)), False, valid)
            send(1, region, slot, (other, s), True, valid)

        def land(piece, zz, q, valid, core=None):
            spot = c if core is None else core
            when(
                valid,
                lambda: arrived(
                    1, region_of(piece, zz, q, spot), slot_of(piece, zz, q), core is not None
                ),
            )

        def planes(d):
            if d == 0:
                return [(z, None, 0)]
            return [(z - d, z >= d, 1), (z + d, z + d < line, -1)]

        def each(d, spots, q_first=True, **where):
            for q in range(cuts):
                for zz, valid, step in planes(d):
                    for a, b in spots:
                        piece = sector_at(a, b)
                        land(piece, zz, q, valid)
                        put(piece, zz, q, valid, **where)

        def from_line_step(d):
            for q in range(cuts):
                for zz, valid, step in planes(d):
                    land(s, zz, q, valid)
                    put(s, zz, q, valid, to_line=(step,), to_first=True, to_second=True)

        side_one = [(a, 0) for a in range(1, nx)]
        rest = [(a, b) for a in range(nx) for b in range(1, ny)]
        for q in range(cuts):
            put(s, z, q, None, to_line=(1, -1), to_first=True, to_second=True)
        for d in range(1, line + 2):
            if d < line:
                from_line_step(d)
            if d - 1 < line:
                each(d - 1, side_one, to_second=True)
            if 0 <= d - 2 < line:
                each(d - 2, rest)
        for d in range(line):
            for zz, valid, step in planes(d):
                for q in range(cuts):
                    for a, b in [(0, 0)] + elsewhere:
                        land(sector_at(a, b), zz, q, valid, core=1 - c)
        drain()

    def pair_copy(stage, g):
        span = pl.ds(g * group, group)
        return pltpu.make_async_remote_copy(
            src_ref=partial.at[stage, span, :, 1 - c],
            dst_ref=from_core.at[stage, span],
            send_sem=pair_send.at[stage, g],
            recv_sem=pair_recv.at[stage, g],
            device_id=(other, s),
            device_id_type=MESH,
        )

    def line_copy(stage, g, j):
        span = pl.ds(g * group, group)
        return pltpu.make_async_remote_copy(
            src_ref=chip_sum.at[stage, z_at(j), span],
            dst_ref=from_line.at[stage, z, span],
            send_sem=line_send.at[stage, g, j],
            recv_sem=line_recv.at[stage, g, z],
            device_id=(2 * z_at(j) + c, s),
            device_id_type=MESH,
        )

    def line_landed(stage, g, j):
        span = pl.ds(g * group, group)
        pltpu.make_async_remote_copy(
            src_ref=chip_sum.at[stage, z, span],
            dst_ref=from_line.at[stage, z_at(j), span],
            send_sem=line_send.at[stage, g, j],
            recv_sem=line_recv.at[stage, g, z_at(j)],
            device_id=(2 * z_at(j) + c, s),
            device_id_type=MESH,
        ).wait_recv()

    def operate(stage, with_sums):
        def finish(g):
            pair_copy(stage, g).wait_recv()
            for i in range(group):
                k = g * group + i
                both = partial[stage, k, :, pl.ds(c, 1)].reshape(line, rows, width)
                both = both + from_core[stage, k]
                chip_sum[stage, :, k] = both.astype(jnp.bfloat16)
            for j in range(1, line):
                line_copy(stage, g, j).start()

        def step(g, sums):
            for i in range(group):
                k = g * group + i
                total = None
                for b in range(bonds):
                    picked = pool[stage, source_ref[b, s * blocks + k]]
                    half = jnp.dot(
                        left[b, k], picked, preferred_element_type=jnp.float32
                    ).astype(jnp.bfloat16)
                    term = lax.dot_general(
                        half,
                        right[b, k],
                        (((1,), (1,)), ((), ())),
                        preferred_element_type=jnp.float32,
                    )
                    total = term if total is None else total + term
                total = jnp.where(keep_of(k), total, jnp.zeros_like(total))
                if with_sums:
                    own = pool[0, s * blocks + k].astype(jnp.float32)
                    sums = (sums[0] + fold(total * own), sums[1] + fold(total * total))
                partial[stage, k] = total.reshape(line, 2, rows, width)
            pair_copy(stage, g).start()

            @pl.when(g >= LAG)
            def _():
                finish(g - LAG)

            return sums

        zero = jnp.zeros((8, LANES), jnp.float32)
        sums = lax.fori_loop(0, groups, step, (zero, zero) if with_sums else (zero,))

        def last():
            for g in range(max(groups - LAG, 0), groups):
                finish(g)

        return sums, last

    def collect(stage):
        for g in range(groups):
            for j in range(1, line):
                line_landed(stage, g, j)
        mine = partial[stage, :, pl.ds(z, 1), pl.ds(c, 1)].reshape(blocks, rows, width)
        mine = mine + from_core[stage, :, pl.ds(z, 1)].reshape(blocks, rows, width)
        for j in range(1, line):
            piece = from_line[stage, pl.ds(z_at(j), 1)].reshape(blocks, rows, width)
            mine = mine + piece.astype(jnp.float32)
        for g in range(groups):
            pair_copy(stage, g).wait_send()
            for j in range(1, line):
                line_copy(stage, g, j).wait_send()
        return mine

    def term_copy(stage, j):
        return pltpu.make_async_remote_copy(
            src_ref=term_out.at[stage],
            dst_ref=term_in.at[stage, j],
            send_sem=term_send.at[stage, j],
            recv_sem=term_recv.at[stage, j],
            device_id=(lax.rem(t + j, terms), s),
            device_id_type=MESH,
        )

    def sector_copy(stage, j):
        return pltpu.make_async_remote_copy(
            src_ref=sector_out.at[stage],
            dst_ref=sector_in.at[stage, j],
            send_sem=sector_send.at[stage, j],
            recv_sem=sector_recv.at[stage, j],
            device_id=(t, lax.rem(s + j, sectors)),
            device_id_type=MESH,
        )

    def share_start(stage, tiles):
        lines = [jnp.sum(tile, axis=0, keepdims=True) for tile in tiles]
        lines.append(jnp.zeros((8 - len(tiles), LANES), jnp.float32))
        term_out[stage] = jnp.concatenate(lines, axis=0)
        for j in range(1, terms):
            term_copy(stage, j).start()

    def share_turn(stage):
        value = term_out[stage]
        for j in range(1, terms):
            term_copy(stage, j).wait_recv()
            value = value + term_in[stage, j]
        sector_out[stage] = value
        for j in range(1, sectors):
            sector_copy(stage, j).start()

    def share_end(stage):
        value = sector_out[stage]
        for j in range(1, sectors):
            sector_copy(stage, j).wait_recv()
            value = value + sector_in[stage, j]
        for j in range(1, terms):
            term_copy(stage, j).wait_send()
        for j in range(1, sectors):
            sector_copy(stage, j).wait_send()
        return jnp.sum(value, axis=1, keepdims=True)

    gather_wave()
    loads[1].wait()
    loads[2].wait()

    sums, last = operate(0, True)
    my_rows = pl.ds(pl.multiple_of(t * rows, rows), rows)
    own = pool[0, pl.ds(s * blocks, blocks), my_rows, :].astype(jnp.float32)
    share_start(0, (sums[0], sums[1], fold(own * own)))
    last()
    share_turn(0)
    first = collect(0)
    first_ref[...] = first
    whole = share_end(0)
    count = float(sectors * blocks * width * width)
    ratio = whole[0:1] / whole[2:3]
    early = jnp.maximum(lax.rsqrt(whole[1:2] / count + epsilon), 1e-18)
    residual = first - ratio * own
    pool[1, pl.ds(s * blocks, blocks), my_rows, :] = (residual * early).astype(jnp.bfloat16)
    gather_next()
    share_start(1, (fold(residual * residual),))

    _, last = operate(1, False)
    last()
    share_turn(1)
    second = collect(1)
    spread = share_end(1)[0:1]
    second_ref[...] = second * (lax.rsqrt(spread / count + epsilon) / early)


def hand_over(first_in, second_in, first_ref, second_ref):
    first_ref[...] = first_in[...]
    second_ref[...] = second_in[...]


def body(dims, wavefunction, left_env, right_env, source, block_size):
    terms, sectors, blocks, bonds, width = dims
    line = terms // 2
    rows = width // terms
    groups = blocks // (GROUP if blocks % GROUP == 0 else 1)
    nx, ny = grid_of(sectors)
    piece = jax.ShapeDtypeStruct((blocks, rows, width), jnp.float32)
    dma = pltpu.SemaphoreType.DMA
    pieces = sectors * max(line * CUTS, blocks)
    sends = CUTS * 2 * line * (nx + nx * ny + sectors + 2) + blocks * (nx + ny + nx * ny + 2 * sectors)
    results = pl.pallas_call(
        functools.partial(kernel, dims),
        out_shape=(piece, piece),
        in_specs=[pl.BlockSpec(memory_space=pltpu.SMEM)] * 2
        + [pl.BlockSpec(memory_space=pl.ANY)] * 3,
        out_specs=(pl.BlockSpec(memory_space=pltpu.VMEM),) * 2,
        scratch_shapes=[
            pltpu.VMEM((blocks, width, width), jnp.bfloat16),
            pltpu.VMEM((bonds, blocks, width, width), jnp.bfloat16),
            pltpu.VMEM((bonds, blocks, width, width), jnp.bfloat16),
            pltpu.VMEM((2, sectors * blocks, width, width), jnp.bfloat16),
            pltpu.VMEM((2, blocks, line, 2, rows, width), jnp.float32),
            pltpu.VMEM((2, blocks, line, rows, width), jnp.float32),
            pltpu.VMEM((2, line, blocks, rows, width), jnp.bfloat16),
            pltpu.VMEM((2, line, blocks, rows, width), jnp.bfloat16),
            pltpu.VMEM((2, 8, LANES), jnp.float32),
            pltpu.VMEM((2, terms, 8, LANES), jnp.float32),
            pltpu.VMEM((2, 8, LANES), jnp.float32),
            pltpu.VMEM((2, sectors, 8, LANES), jnp.float32),
            dma((3,)),
            dma((sends,)),
            dma((2, pieces)),
            dma((2, pieces)),
            dma((2, groups)),
            dma((2, groups)),
            dma((2, groups, line)),
            dma((2, groups, line)),
            dma((2, terms)),
            dma((2, terms)),
            dma((2, sectors)),
            dma((2, sectors)),
        ],
        compiler_params=pltpu.CompilerParams(
            collective_id=0, has_side_effects=True, vmem_limit_bytes=60 * 1024 * 1024
        ),
    )(source, block_size.T, wavefunction, left_env, right_env)
    return pl.pallas_call(
        hand_over,
        out_shape=(piece, piece),
        in_specs=[pl.BlockSpec(memory_space=pltpu.VMEM)] * 2,
        out_specs=(pl.BlockSpec(memory_space=pltpu.VMEM),) * 2,
    )(*results)


def solution(mesh):
    terms, sectors = mesh.shape["term"], mesh.shape["sector"]

    def local(wavefunction, left_env, right_env, source, block_size):
        blocks, width = wavefunction.shape[0], wavefunction.shape[1]
        dims = (terms, sectors, blocks, source.shape[0], width)
        return body(dims, wavefunction, left_env, right_env, source, block_size)

    placed = (
        P("sector", None, None),
        P("term", "sector", None, None),
        P("term", "sector", None, None),
        P("term", None),
        P("sector", None),
    )
    return jax.shard_map(
        local,
        mesh=mesh,
        in_specs=placed,
        out_specs=(P("sector", "term", None), P("sector", "term", None)),
        check_vma=False,
    )
```
